32 devices in a mesh: chain: 8 (over z, core), bond: 4 (over y, x).
Axes of the slice: x: 2, y: 2, z: 4, core: 2. Of those that a mesh axis runs over, the one named last changes fastest.
Arguments:
- site_tensors: float32 [32, 256, 2, 256], P('chain', 'bond'), may hold values from -20 to 20
- bond_gates: float32 [32, 4, 4], P('chain'), may hold values from -1.5 to 2.5
Outputs:
- state: float32 [32, 256, 2, 256], P('chain', 'bond')
- profile: float32 [32], P('chain')
The draws below stay inside these ranges and needn't reach their ends.
All inputs are finite; a program needn't handle non-finite values.
Results may differ from the reference program's by a relative error of at most 0.0002.
Values sent between devices are 32-bit elements; how exact they have to be, the bound alone decides.
A program may use at most 64 MiB of HBM per device.

```python
import math
import jax
import jax.numpy as jnp
from jax import lax

CHI = 256
NS_ITERS = 3
SITES = 32


def draw_site_tensors(key, part):
    key_base = jax.random.fold_in(key, 11)
    shape = (SITES, CHI, 2, CHI)
    base = jnp.clip(jax.random.normal(key_base, shape, jnp.float32), -6.0, 6.0)
    ramp = jnp.exp(-2.0 * jnp.arange(SITES, dtype=jnp.float32) / SITES)
    return base * ramp[:, None, None, None]


def draw_bond_gates(key, part):
    key_noise = jax.random.fold_in(key, 21)
    noise = 0.3 * jnp.clip(jax.random.normal(key_noise, (SITES, 4, 4), jnp.float32), -4.0, 4.0)
    return jnp.eye(4, dtype=jnp.float32)[None, :, :] + noise


def setup_inputs(seed: int = 0) -> dict:
    key_list = jax.random.split(jax.random.key(seed), 3)
    return {
        "site_tensors": draw_site_tensors(jax.random.fold_in(key_list[2], 71), 0),
        "bond_gates": draw_bond_gates(jax.random.fold_in(key_list[2], 71), 0),
    }


epsilon = 1e-06
exact = lax.Precision.HIGHEST

def bond_update(operands):
    left, right, gate = operands
    width = left.shape[0]
    two_site = jnp.einsum('asm,mtb->astb', left, right, precision=exact) / math.sqrt(width)
    gated = jnp.einsum('stuv,auvb->astb', gate.reshape(2, 2, 2, 2), two_site, precision=exact)
    matrix = gated.reshape(2 * width, 2 * width)
    projected = jnp.dot(matrix, right.reshape(width, 2 * width).T, precision=exact)
    squares = jnp.sum(projected * projected)
    iterate = projected / jnp.sqrt(squares + epsilon)
    for repeat in range(NS_ITERS):
        gram = jnp.dot(iterate.T, iterate, precision=exact)
        iterate = 1.5 * iterate - 0.5 * jnp.dot(iterate, gram, precision=exact)
    carried = jnp.dot(iterate.T, matrix, precision=exact)
    scale_norm = jnp.sqrt(jnp.mean(carried * carried) + epsilon)
    new_left = (math.sqrt(2 * width) * iterate).reshape(width, 2, width)
    new_right = (carried / scale_norm).reshape(width, 2, width)
    return (new_left, new_right, jnp.log(scale_norm))

def reference(site_tensors, bond_gates):
    sites = site_tensors.shape[0]
    new_left, new_right, weights_even = lax.map(bond_update, (site_tensors[0::2], site_tensors[1::2], bond_gates[0::2]))
    half_state = jnp.stack([new_left, new_right], axis=1).reshape(site_tensors.shape)
    rolled = jnp.roll(half_state, -1, axis=0)
    new_left, new_right, weights_odd = lax.map(bond_update, (half_state[1::2], rolled[1::2], bond_gates[1::2]))
    even_sites = jnp.roll(new_right, 1, axis=0)
    state = jnp.stack([even_sites, new_left], axis=1).reshape(site_tensors.shape)
    weights = jnp.stack([weights_even, weights_odd], axis=1).reshape(sites)
    profile = jnp.cumsum(weights) / sites
    return (state, profile)
```

```python
import functools
import math

import jax
import jax.numpy as jnp
from jax import lax
from jax.experimental import pallas as pl
from jax.experimental.pallas import tpu as pltpu
from jax.sharding import PartitionSpec as P

NS_ITERS = 3
RING = 4
CHUNKS = 4
LANES = 128
EPSILON = 1e-06


def split(value):
    high = value.astype(jnp.bfloat16)
    low = (value - high.astype(jnp.float32)).astype(jnp.bfloat16)
    return (high, low)


def times(a, b):
    (ah, al), (bh, bl) = (a, b)
    return jnp.dot(
        jnp.concatenate([ah, ah, al], axis=1),
        jnp.concatenate([bh, bl, bh], axis=0),
        preferred_element_type=jnp.float32,
    )


def times_transposed(a, b):
    (ah, al), (bh, bl) = (a, b)
    return lax.dot_general(
        jnp.concatenate([ah, ah, al], axis=1),
        jnp.concatenate([bh, bl, bh], axis=1),
        (((1,), (1,)), ((), ())),
        preferred_element_type=jnp.float32,
    )


def update(left, right, gate, on_left):
    width = right.shape[0]
    right_split = split(right)
    theta = times(split(left), right_split) * (1.0 / math.sqrt(width))
    theta = [[theta[u * width:(u + 1) * width, v * width:(v + 1) * width] for v in range(2)] for u in range(2)]
    rows = []
    for s in range(2):
        row = []
        for t in range(2):
            total = None
            for u in range(2):
                for v in range(2):
                    factor = gate[2 * s + t:2 * s + t + 1, 2 * u + v:2 * u + v + 1]
                    term = factor * theta[u][v]
                    total = term if total is None else total + term
            row.append(total)
        rows.append(jnp.concatenate(row, axis=1))
    matrix = split(jnp.concatenate(rows, axis=0))
    projected = times_transposed(matrix, right_split)
    squares = jnp.sum(projected * projected, keepdims=True)
    iterate = projected * (1.0 / jnp.sqrt(squares + EPSILON))
    turned = split(iterate.T)
    iterate = split(iterate)
    gram = times_transposed(turned, turned)
    eye = jnp.where(
        lax.broadcasted_iota(jnp.int32, gram.shape, 0) == lax.broadcasted_iota(jnp.int32, gram.shape, 1),
        jnp.float32(1.5),
        jnp.float32(0.0),
    )
    carried = times(turned, matrix)
    factor = None
    for repeat in range(NS_ITERS):
        step = eye - 0.5 * gram
        factor = step if factor is None else times(split(factor), split(step))
        if repeat < NS_ITERS - 1:
            gram_split = split(gram)
            once = 1.5 * gram - 0.5 * times(gram_split, gram_split)
            gram = 1.5 * once - 0.5 * times(split(once), gram_split)
    factor = split(factor)
    on_left(math.sqrt(2 * width) * times(iterate, factor))
    carried = times(factor, split(carried))
    mean = jnp.sum(carried * carried, keepdims=True) * (1.0 / carried.size)
    scale_norm = jnp.sqrt(mean + EPSILON)
    return (carried * (1.0 / scale_norm), jnp.log(scale_norm))


def order(place):
    return place + (place // 2) * (1 - 2 * (place % 2))


def kernel(
    chains, bonds, rows, width,
    x_ref, gates_ref, out_ref, profile_ref,
    inbuf, gates, xbuf, recv, obuf, wall,
    g_send, g_recv, f_send, f_recv, gate_send, gate_recv,
    m_send, m_recv, h_send, h_recv, o_send, o_recv, w_send, w_recv,
):
    chain, bond = (lax.axis_index("chain"), lax.axis_index("bond"))
    slabs = chains // 2
    slab, core = (chain // 2, chain % 2)
    replica, ring = (bond // RING, order(bond % RING))
    tall = rows * 4
    height = width // CHUNKS
    sibling = {"chain": 2 * slab + 1 - core, "bond": bond}

    def remote(src, dst, send, recv_sem, chain_to, bond_to):
        return pltpu.make_async_remote_copy(
            src_ref=src, dst_ref=dst, send_sem=send, recv_sem=recv_sem,
            device_id={"chain": chain_to, "bond": bond_to},
            device_id_type=pl.DeviceIdType.MESH,
        )

    def landed(ref, sem):
        pltpu.make_async_copy(ref, ref, sem).wait()

    gathers = []
    for j in range(2):
        for r in range(bonds // RING):
            bond_to = r * RING + order(2 * core + j)
            for i in range(2):
                src = x_ref.at[pl.ds((2 * j + i) * tall, tall)]
                dst = inbuf.at[i, pl.ds(bond * tall, tall)]
                copy = remote(src, dst, g_send.at[j, r, i], g_recv.at[bond], 2 * slab + i, bond_to)
                here = pltpu.make_async_copy(src, dst, g_recv.at[bond])
                mine = jnp.logical_and(core == i, bond_to == bond)
                gathers.append((copy, here, mine))
                pl.when(mine)(here.start)
                pl.when(jnp.logical_not(mine))(copy.start)
    gate_here = pltpu.make_async_copy(gates_ref, gates.at[core], gate_recv.at[core])
    gate_here.start()
    gate_copy = remote(gates_ref, gates.at[core], gate_send, gate_recv.at[core], sibling["chain"], bond)
    gate_copy.start()

    forwards = []
    for d in range(bonds):
        origin = lax.rem(bond + d, bonds)
        piece = inbuf.at[core, pl.ds(origin * tall, tall)]
        landed(piece, g_recv.at[origin])
        copy = remote(piece, piece, f_send.at[origin], f_recv.at[origin], sibling["chain"], bond)
        copy.start()
        forwards.append(copy)
    for d in range(bonds):
        origin = lax.rem(bond + d, bonds)
        landed(inbuf.at[1 - core, pl.ds(origin * tall, tall)], f_recv.at[origin])
    landed(gates.at[0], gate_recv.at[0])
    landed(gates.at[1], gate_recv.at[1])

    def spin(i, s):
        return jnp.concatenate(
            [inbuf[i, pl.ds(2 * t + s, width, stride=4), :] for t in range(2)], axis=1
        )

    passed = []

    def send_left(value):
        xbuf[0] = value[:width]
        xbuf[1] = value[width:]
        before = lax.rem(ring + RING - 1, RING)
        slab_to = lax.rem(slab + slabs - jnp.where(ring == 0, 1, 0), slabs)
        bond_to = replica * RING + order(before)
        for q in range(CHUNKS):
            part = pl.ds(q * height, height)
            copy = remote(
                xbuf.at[core, part], recv.at[core, part], m_send.at[q], m_recv.at[q],
                2 * slab_to + core, bond_to,
            )
            copy.start()
            passed.append(copy)

    block = ring // 2
    left = jnp.concatenate([spin(0, 0), spin(0, 1)], axis=0)
    right = jnp.concatenate([spin(1, 0), spin(1, 1)], axis=1)
    new_right, weight_even = update(left, right, gates[block, 2 * (ring % 2)], send_left)

    for q in range(CHUNKS):
        part = recv.at[core, pl.ds(q * height, height)]
        landed(part, m_recv.at[q])
        copy = remote(part, part, h_send.at[q], h_recv.at[q], sibling["chain"], bond)
        copy.start()
        forwards.append(copy)
    for q in range(CHUNKS):
        landed(recv.at[1 - core, pl.ds(q * height, height)], h_recv.at[q])

    outs = []

    def put(h, value_of):
        for s in range(2):
            for t in range(2):
                obuf[h, pl.ds(2 * t + s, width, stride=4), :] = value_of(s, t)
        site = lax.rem(slab * 2 * RING + 2 * ring + 1 + h, 4 * chains)
        chain_to, slot = (site // 4, site % 4)
        for j in range(2):
            bond_to = replica * RING + 2 * j + core
            src = obuf.at[h, pl.ds(bond_to * tall, tall)]
            dst = out_ref.at[pl.ds(slot * tall, tall)]
            copy = remote(src, dst, o_send.at[h, j], o_recv.at[slot], chain_to, bond_to)
            here = pltpu.make_async_copy(src, dst, o_recv.at[slot])
            mine = jnp.logical_and(chain_to == chain, bond_to == bond)
            outs.append((copy, mine))
            pl.when(mine)(here.start)
            pl.when(jnp.logical_not(mine))(copy.start)

    def put_left(value):
        put(0, lambda s, t: value[s * width:(s + 1) * width, t * LANES:(t + 1) * LANES])

    left = jnp.concatenate([new_right[:, :width], new_right[:, width:]], axis=0)
    right = jnp.concatenate([recv[0], recv[1]], axis=1)
    new_right, weight_odd = update(left, right, gates[block, 2 * (ring % 2) + 1], put_left)
    put(1, lambda s, t: new_right[:, s * width + t * LANES:s * width + (t + 1) * LANES])

    row = lax.broadcasted_iota(jnp.int32, (8, LANES), 0)
    lane = lax.broadcasted_iota(jnp.int32, (8, LANES), 1)
    own = wall.at[slab * RING + ring]
    own[...] = jnp.where(row == 0, weight_even, weight_odd)
    weights = []
    for dz in range(slabs):
        for dk in range(RING):
            if dz == 0 and dk == 0:
                continue
            chain_to = 2 * lax.rem(slab + dz, slabs) + core
            bond_to = replica * RING + order(lax.rem(ring + dk, RING))
            at = dz * RING + dk
            copy = remote(own, own, w_send.at[at], w_recv.at[at], chain_to, bond_to)
            copy.start()
            weights.append((copy, dz, dk))
    for copy, dz, dk in weights:
        source = lax.rem(slab + slabs - dz, slabs) * RING + lax.rem(ring + RING - dk, RING)
        landed(wall.at[source], w_recv.at[dz * RING + dk])
    total = jnp.zeros((8, LANES), jnp.float32)
    for e in range(slabs * RING):
        counted = jnp.logical_and(row < 2, 2 * e + row <= 4 * chain + lane)
        total = total + jnp.where(counted, wall[e], 0.0)
    running = jnp.sum(total, axis=0, keepdims=True) * (1.0 / (4 * chains))
    profile_ref[...] = jnp.broadcast_to(running, (8, LANES))

    for slot in range(4):
        landed(out_ref.at[pl.ds(slot * tall, tall)], o_recv.at[slot])
    for copy, here, mine in gathers:
        pl.when(jnp.logical_not(mine))(copy.wait_send)
    gate_copy.wait_send()
    for copy in forwards + passed + [c for c, dz, dk in weights]:
        copy.wait_send()
    for copy, mine in outs:
        pl.when(jnp.logical_not(mine))(copy.wait_send)


def per_device(chains, bonds, site_tensors, bond_gates):
    sites, rows, spins, width = site_tensors.shape
    assert sites == 4 and spins == 2 and width == 2 * LANES and bonds % RING == 0 and chains % 2 == 0
    cut = (sites, rows, spins, width // LANES, LANES)
    flat = site_tensors.reshape(cut).transpose(0, 1, 3, 2, 4).reshape(sites * rows * 4, LANES)
    slabs = chains // 2
    dma = pltpu.SemaphoreType.DMA
    out, profile = pl.pallas_call(
        functools.partial(kernel, chains, bonds, rows, width),
        out_shape=(
            jax.ShapeDtypeStruct(flat.shape, jnp.float32),
            jax.ShapeDtypeStruct((8, LANES), jnp.float32),
        ),
        in_specs=[pl.BlockSpec(memory_space=pl.ANY)] * 2,
        out_specs=(pl.BlockSpec(memory_space=pl.ANY), pl.BlockSpec(memory_space=pltpu.VMEM)),
        scratch_shapes=[
            pltpu.VMEM((2, 4 * width, LANES), jnp.float32),
            pltpu.VMEM((2,) + bond_gates.shape, jnp.float32),
            pltpu.VMEM((2, width, width), jnp.float32),
            pltpu.VMEM((2, width, width), jnp.float32),
            pltpu.VMEM((2, 4 * width, LANES), jnp.float32),
            pltpu.VMEM((slabs * RING, 8, LANES), jnp.float32),
            dma((2, bonds // RING, 2)), dma((bonds,)),
            dma((bonds,)), dma((bonds,)),
            dma, dma((2,)),
            dma((CHUNKS,)), dma((CHUNKS,)),
            dma((CHUNKS,)), dma((CHUNKS,)),
            dma((2, 2)), dma((4,)),
            dma((slabs * RING,)), dma((slabs * RING,)),
        ],
        compiler_params=pltpu.CompilerParams(
            has_side_effects=True, vmem_limit_bytes=48 * 1024 * 1024
        ),
    )(flat, bond_gates)
    cut = (sites, rows, width // LANES, spins, LANES)
    state = out.reshape(cut).transpose(0, 1, 3, 2, 4).reshape(site_tensors.shape)
    return (state, profile[0, :sites])


def solution(mesh):
    chains, bonds = (mesh.shape["chain"], mesh.shape["bond"])
    return jax.shard_map(
        functools.partial(per_device, chains, bonds),
        mesh=mesh,
        in_specs=(P("chain", "bond", None, None), P("chain", None, None)),
        out_specs=(P("chain", "bond", None, None), P("chain")),
        check_vma=False,
    )
```

```python
import functools
import math

import jax
import jax.numpy as jnp
from jax import lax
from jax.experimental import pallas as pl
from jax.experimental.pallas import tpu as pltpu
from jax.sharding import PartitionSpec as P

NS_ITERS = 3
RING = 4
CHUNKS = 4
LANES = 128
EPSILON = 1e-06


def split(value):
    high = value.astype(jnp.bfloat16)
    low = (value - high.astype(jnp.float32)).astype(jnp.bfloat16)
    return (high, low)


def times(a, b):
    (ah, al), (bh, bl) = (a, b)
    return jnp.dot(
        jnp.concatenate([ah, ah, al], axis=1),
        jnp.concatenate([bh, bl, bh], axis=0),
        preferred_element_type=jnp.float32,
    )


def times_transposed(a, b):
    (ah, al), (bh, bl) = (a, b)
    return lax.dot_general(
        jnp.concatenate([ah, ah, al], axis=1),
        jnp.concatenate([bh, bl, bh], axis=1),
        (((1,), (1,)), ((), ())),
        preferred_element_type=jnp.float32,
    )


def update(right, lefts, gate, on_left):
    width = right.shape[0]
    right_split = split(right)
    groups = []
    projected = []
    for left in lefts:
        left = left()
        r = left.shape[0] // 2
        theta = times(split(left), right_split) * (1.0 / math.sqrt(width))
        theta = [[theta[u * r:(u + 1) * r, v * width:(v + 1) * width] for v in range(2)] for u in range(2)]
        rows = []
        for s in range(2):
            row = []
            for t in range(2):
                total = None
                for u in range(2):
                    for v in range(2):
                        factor = gate[2 * s + t:2 * s + t + 1, 2 * u + v:2 * u + v + 1]
                        term = factor * theta[u][v]
                        total = term if total is None else total + term
                row.append(total)
            rows.append(jnp.concatenate(row, axis=1))
        group = split(jnp.concatenate(rows, axis=0))
        groups.append(group)
        projected.append(times_transposed(group, right_split))
    matrix = tuple(jnp.concatenate(part, axis=0) for part in zip(*groups))
    projected = jnp.concatenate(projected, axis=0)
    squares = jnp.sum(projected * projected, keepdims=True)
    iterate = projected * (1.0 / jnp.sqrt(squares + EPSILON))
    turned = split(iterate.T)
    iterate = split(iterate)
    gram = times_transposed(turned, turned)
    eye = jnp.where(
        lax.broadcasted_iota(jnp.int32, gram.shape, 0) == lax.broadcasted_iota(jnp.int32, gram.shape, 1),
        jnp.float32(1.5),
        jnp.float32(0.0),
    )
    carried = times(turned, matrix)
    factor = None
    for repeat in range(NS_ITERS):
        step = eye - 0.5 * gram
        factor = step if factor is None else times(split(factor), split(step))
        if repeat < NS_ITERS - 1:
            gram_split = split(gram)
            once = 1.5 * gram - 0.5 * times(gram_split, gram_split)
            gram = 1.5 * once - 0.5 * times(split(once), gram_split)
    factor = split(factor)
    on_left(math.sqrt(2 * width) * times(iterate, factor))
    carried = times(factor, split(carried))
    mean = jnp.sum(carried * carried, keepdims=True) * (1.0 / carried.size)
    scale_norm = jnp.sqrt(mean + EPSILON)
    return (carried * (1.0 / scale_norm), jnp.log(scale_norm))


def order(place):
    return place + (place // 2) * (1 - 2 * (place % 2))


def kernel(
    chains, bonds, rows, width,
    x_ref, gates_ref, out_ref, profile_ref,
    slab_sem, ring_sem, fetch_sem, xin, inbuf, gates, xbuf, recv, obuf, wall,
    g_send, g_recv, f_send, f_recv, gate_send, gate_recv,
    m_send, m_recv, h_send, h_recv, o_send, o_recv, w_send, w_recv,
):
    chain, bond = (lax.axis_index("chain"), lax.axis_index("bond"))
    slabs = chains // 2
    slab, core = (chain // 2, chain % 2)
    replica, ring = (bond // RING, order(bond % RING))
    tall = rows * 4
    height = width // CHUNKS
    sibling = {"chain": 2 * slab + 1 - core, "bond": bond}

    def remote(src, dst, send, recv_sem, chain_to, bond_to):
        return pltpu.make_async_remote_copy(
            src_ref=src, dst_ref=dst, send_sem=send, recv_sem=recv_sem,
            device_id={"chain": chain_to, "bond": bond_to},
            device_id_type=pl.DeviceIdType.MESH,
        )

    def landed(ref, sem):
        pltpu.make_async_copy(ref, ref, sem).wait()

    fetch = pltpu.make_async_copy(x_ref, xin, fetch_sem)
    fetch.start()
    gate_here = pltpu.make_async_copy(gates_ref, gates.at[core], gate_recv.at[core])
    gate_here.start()
    barrier = pltpu.get_barrier_semaphore()

    def greet(semaphore, chain_to, bond_to):
        to = {"chain": chain_to, "bond": bond_to}
        pl.semaphore_signal(semaphore, inc=1, device_id=to, device_id_type=pl.DeviceIdType.MESH)

    for db in range(1, bonds):
        greet(barrier, 2 * slab + 1, lax.rem(bond + db, bonds))

    @pl.when(core == 0)
    def _():
        greet(barrier, 2 * slab + 1, bond)

    for dz in range(1, slabs):
        for db in range(RING):
            greet(barrier, 2 * lax.rem(slab + dz, slabs), replica * RING + lax.rem(bond + db, RING))

    @pl.when(core == 1)
    def _():
        pl.semaphore_wait(barrier, 2 * bonds - 1)
        greet(slab_sem, 2 * slab, bond)

    @pl.when(core == 0)
    def _():
        pl.semaphore_wait(slab_sem, 1)

    gate_copy = remote(gates_ref, gates.at[core], gate_send, gate_recv.at[core], sibling["chain"], bond)
    gate_copy.start()
    fetch.wait()

    short = tall // 2
    gathers = []
    for i in (1, 0):
        for h in range(2):
            for j in range(2):
                for r in range(bonds // RING):
                    bond_to = r * RING + order(2 * core + j)
                    src = xin.at[pl.ds((2 * j + i) * tall + h * short, short)]
                    dst = inbuf.at[i, pl.ds(bond * tall + h * short, short)]
                    sem = g_recv.at[i, bond]
                    copy = remote(src, dst, g_send.at[i, h, j, r], sem, 2 * slab + h, bond_to)
                    here = pltpu.make_async_copy(src, dst, sem)
                    mine = jnp.logical_and(core == h, bond_to == bond)
                    gathers.append((copy, mine))
                    pl.when(mine)(here.start)
                    pl.when(jnp.logical_not(mine))(copy.start)

    forwards = []
    part = bonds // 2
    first = bond // part

    def receive(i, origins):
        for origin in origins:
            piece = inbuf.at[i, pl.ds(origin * tall + core * short, short)]
            landed(piece, g_recv.at[i, origin])
            copy = remote(
                piece, piece, f_send.at[i, origin], f_recv.at[i, origin], sibling["chain"], bond
            )
            copy.start()
            forwards.append(copy)
        for origin in origins:
            landed(inbuf.at[i, pl.ds(origin * tall + (1 - core) * short, short)], f_recv.at[i, origin])

    def spin(i, s, row, count):
        return jnp.concatenate(
            [inbuf[i, pl.ds(4 * row + 2 * t + s, count, stride=4), :] for t in range(2)], axis=1
        )

    def meet_ring():
        @pl.when(core == 0)
        def _():
            pl.semaphore_wait(barrier, (slabs - 1) * 2 * RING)
            greet(ring_sem, 2 * slab + 1, bond)

        @pl.when(core == 1)
        def _():
            pl.semaphore_wait(ring_sem, 1)

    passed = []

    def send_left(value):
        for g in range(2):
            for s in range(2):
                here = pl.ds((first + g * (1 - 2 * first)) * half, half)
                xbuf[s, here] = value[(2 * g + s) * half:(2 * g + s + 1) * half]
        before = lax.rem(ring + RING - 1, RING)
        slab_to = lax.rem(slab + slabs - jnp.where(ring == 0, 1, 0), slabs)
        bond_to = replica * RING + order(before)
        for q in range(CHUNKS):
            part = pl.ds(q * height, height)
            copy = remote(
                xbuf.at[core, part], recv.at[core, part], m_send.at[q], m_recv.at[q],
                2 * slab_to + core, bond_to,
            )
            copy.start()
            passed.append(copy)

    block = ring // 2
    half = width // 2

    def left_rows(g):
        which = first + g * (1 - 2 * first)
        receive(0, [which * part + lax.rem(bond + d, part) for d in range(part)])
        return jnp.concatenate([spin(0, s, which * half, half) for s in range(2)], axis=0)

    meet_ring()
    receive(1, [lax.rem(bond + d, bonds) for d in range(bonds)])
    landed(gates.at[0], gate_recv.at[0])
    landed(gates.at[1], gate_recv.at[1])
    right = jnp.concatenate([spin(1, s, 0, width) for s in range(2)], axis=1)
    lefts = [functools.partial(left_rows, g) for g in range(2)]
    new_right, weight_even = update(right, lefts, gates[block, 2 * (ring % 2)], send_left)

    for q in range(CHUNKS):
        part = recv.at[core, pl.ds(q * height, height)]
        landed(part, m_recv.at[q])
        copy = remote(part, part, h_send.at[q], h_recv.at[q], sibling["chain"], bond)
        copy.start()
        forwards.append(copy)
    for q in range(CHUNKS):
        landed(recv.at[1 - core, pl.ds(q * height, height)], h_recv.at[q])

    outs = []

    def put(h, value_of):
        for s in range(2):
            for t in range(2):
                obuf[h, pl.ds(2 * t + s, width, stride=4), :] = value_of(s, t)
        site = lax.rem(slab * 2 * RING + 2 * ring + 1 + h, 4 * chains)
        chain_to, slot = (site // 4, site % 4)
        for j in range(2):
            bond_to = replica * RING + 2 * j + core
            src = obuf.at[h, pl.ds(bond_to * tall, tall)]
            dst = out_ref.at[pl.ds(slot * tall, tall)]
            copy = remote(src, dst, o_send.at[h, j], o_recv.at[slot], chain_to, bond_to)
            here = pltpu.make_async_copy(src, dst, o_recv.at[slot])
            mine = jnp.logical_and(chain_to == chain, bond_to == bond)
            outs.append((copy, mine))
            pl.when(mine)(here.start)
            pl.when(jnp.logical_not(mine))(copy.start)

    def put_left(value):
        put(0, lambda s, t: value[s * width:(s + 1) * width, t * LANES:(t + 1) * LANES])

    left = jnp.concatenate([new_right[:, :width], new_right[:, width:]], axis=0)
    right = jnp.concatenate([recv[0], recv[1]], axis=1)
    new_right, weight_odd = update(right, [lambda: left], gates[block, 2 * (ring % 2) + 1], put_left)

    row = lax.broadcasted_iota(jnp.int32, (8, LANES), 0)
    lane = lax.broadcasted_iota(jnp.int32, (8, LANES), 1)
    own = wall.at[slab * RING + ring]
    own[...] = jnp.where(row == 0, weight_even, weight_odd)
    weights = []
    for dz in range(slabs):
        for dk in range(RING):
            if dz == 0 and dk == 0:
                continue
            chain_to = 2 * lax.rem(slab + dz, slabs) + core
            bond_to = replica * RING + order(lax.rem(ring + dk, RING))
            at = dz * RING + dk
            copy = remote(own, own, w_send.at[at], w_recv.at[at], chain_to, bond_to)
            copy.start()
            weights.append((copy, dz, dk))
    put(1, lambda s, t: new_right[:, s * width + t * LANES:s * width + (t + 1) * LANES])
    for copy, dz, dk in weights:
        source = lax.rem(slab + slabs - dz, slabs) * RING + lax.rem(ring + RING - dk, RING)
        landed(wall.at[source], w_recv.at[dz * RING + dk])
    total = jnp.zeros((8, LANES), jnp.float32)
    for e in range(slabs * RING):
        counted = jnp.logical_and(row < 2, 2 * e + row <= 4 * chain + lane)
        total = total + jnp.where(counted, wall[e], 0.0)
    running = jnp.sum(total, axis=0, keepdims=True) * (1.0 / (4 * chains))
    profile_ref[...] = jnp.broadcast_to(running, (8, LANES))

    for slot in range(4):
        landed(out_ref.at[pl.ds(slot * tall, tall)], o_recv.at[slot])
    for copy, mine in gathers:
        pl.when(jnp.logical_not(mine))(copy.wait_send)
    gate_copy.wait_send()
    for copy in forwards + passed + [c for c, dz, dk in weights]:
        copy.wait_send()
    for copy, mine in outs:
        pl.when(jnp.logical_not(mine))(copy.wait_send)


def per_device(chains, bonds, site_tensors, bond_gates):
    sites, rows, spins, width = site_tensors.shape
    assert sites == 4 and spins == 2 and width == 2 * LANES and bonds % RING == 0 and chains % 2 == 0
    cut = (sites, rows, spins, width // LANES, LANES)
    flat = site_tensors.reshape(cut).transpose(0, 1, 3, 2, 4).reshape(sites * rows * 4, LANES)
    slabs = chains // 2
    dma = pltpu.SemaphoreType.DMA
    out, profile = pl.pallas_call(
        functools.partial(kernel, chains, bonds, rows, width),
        out_shape=(
            jax.ShapeDtypeStruct(flat.shape, jnp.float32),
            jax.ShapeDtypeStruct((8, LANES), jnp.float32),
        ),
        in_specs=[pl.BlockSpec(memory_space=pltpu.HBM)] * 2,
        out_specs=(pl.BlockSpec(memory_space=pl.ANY), pl.BlockSpec(memory_space=pltpu.VMEM)),
        scratch_shapes=[
            pltpu.SemaphoreType.REGULAR,
            pltpu.SemaphoreType.REGULAR,
            dma,
            pltpu.VMEM(flat.shape, jnp.float32),
            pltpu.VMEM((2, 4 * width, LANES), jnp.float32),
            pltpu.VMEM((2,) + bond_gates.shape, jnp.float32),
            pltpu.VMEM((2, width, width), jnp.float32),
            pltpu.VMEM((2, width, width), jnp.float32),
            pltpu.VMEM((2, 4 * width, LANES), jnp.float32),
            pltpu.VMEM((slabs * RING, 8, LANES), jnp.float32),
            dma((2, 2, 2, bonds // RING)), dma((2, bonds)),
            dma((2, bonds)), dma((2, bonds)),
            dma, dma((2,)),
            dma((CHUNKS,)), dma((CHUNKS,)),
            dma((CHUNKS,)), dma((CHUNKS,)),
            dma((2, 2)), dma((4,)),
            dma((slabs * RING,)), dma((slabs * RING,)),
        ],
        compiler_params=pltpu.CompilerParams(
            has_side_effects=True, collective_id=0, vmem_limit_bytes=67043328
        ),
    )(flat, bond_gates)
    cut = (sites, rows, width // LANES, spins, LANES)
    state = out.reshape(cut).transpose(0, 1, 3, 2, 4).reshape(site_tensors.shape)
    return (state, profile[0, :sites])


def solution(mesh):
    chains, bonds = (mesh.shape["chain"], mesh.shape["bond"])
    return jax.shard_map(
        functools.partial(per_device, chains, bonds),
        mesh=mesh,
        in_specs=(P("chain", "bond", None, None), P("chain", None, None)),
        out_specs=(P("chain", "bond", None, None), P("chain")),
        check_vma=False,
    )
```

```python
import functools
import math

import jax
import jax.numpy as jnp
from jax import lax
from jax.experimental import pallas as pl
from jax.experimental.pallas import tpu as pltpu
from jax.sharding import PartitionSpec as P

NS_ITERS = 3
RING = 4
CHUNKS = 4
LANES = 128
EPSILON = 1e-06


def split(value):
    high = value.astype(jnp.bfloat16)
    low = (value - high.astype(jnp.float32)).astype(jnp.bfloat16)
    return (high, low)


def times(a, b):
    (ah, al), (bh, bl) = (a, b)
    return jnp.dot(
        jnp.concatenate([ah, ah, al], axis=1),
        jnp.concatenate([bh, bl, bh], axis=0),
        preferred_element_type=jnp.float32,
    )


def times_transposed(a, b):
    (ah, al), (bh, bl) = (a, b)
    return lax.dot_general(
        jnp.concatenate([ah, ah, al], axis=1),
        jnp.concatenate([bh, bl, bh], axis=1),
        (((1,), (1,)), ((), ())),
        preferred_element_type=jnp.float32,
    )


def update(right, lefts, gate, on_left):
    width = right.shape[0]
    right_split = split(right)
    groups = []
    projected = []
    for left in lefts:
        left = left()
        r = left.shape[0] // 2
        theta = times(split(left), right_split) * (1.0 / math.sqrt(width))
        theta = [[theta[u * r:(u + 1) * r, v * width:(v + 1) * width] for v in range(2)] for u in range(2)]
        rows = []
        for s in range(2):
            row = []
            for t in range(2):
                total = None
                for u in range(2):
                    for v in range(2):
                        factor = gate[2 * s + t:2 * s + t + 1, 2 * u + v:2 * u + v + 1]
                        term = factor * theta[u][v]
                        total = term if total is None else total + term
                row.append(total)
            rows.append(jnp.concatenate(row, axis=1))
        group = split(jnp.concatenate(rows, axis=0))
        groups.append(group)
        projected.append(times_transposed(group, right_split))
    matrix = tuple(jnp.concatenate(part, axis=0) for part in zip(*groups))
    projected = jnp.concatenate(projected, axis=0)
    squares = jnp.sum(projected * projected, keepdims=True)
    iterate = projected * (1.0 / jnp.sqrt(squares + EPSILON))
    turned = split(iterate.T)
    iterate = split(iterate)
    gram = times_transposed(turned, turned)
    eye = jnp.where(
        lax.broadcasted_iota(jnp.int32, gram.shape, 0) == lax.broadcasted_iota(jnp.int32, gram.shape, 1),
        jnp.float32(1.5),
        jnp.float32(0.0),
    )
    carried = times(turned, matrix)
    factor = None
    for repeat in range(NS_ITERS):
        step = eye - 0.5 * gram
        factor = step if factor is None else times(split(factor), split(step))
        if repeat < NS_ITERS - 1:
            gram_split = split(gram)
            once = 1.5 * gram - 0.5 * times(gram_split, gram_split)
            gram = 1.5 * once - 0.5 * times(split(once), gram_split)
    factor = split(factor)
    on_left(math.sqrt(2 * width) * times(iterate, factor))
    carried = times(factor, split(carried))
    mean = jnp.sum(carried * carried, keepdims=True) * (1.0 / carried.size)
    scale_norm = jnp.sqrt(mean + EPSILON)
    return (carried * (1.0 / scale_norm), jnp.log(scale_norm))


def order(place):
    return place + (place // 2) * (1 - 2 * (place % 2))


def kernel(
    chains, bonds, rows, width,
    x_ref, gates_ref, out_ref, profile_ref,
    slab_sem, ring_sem, fetch_sem, xin, inbuf, gates, xbuf, recv, obuf, wall,
    g_send, g_recv, f_send, f_recv, gate_send, gate_recv,
    m_send, m_recv, h_send, h_recv, o_send, o_recv, w_send, w_recv,
):
    chain, bond = (lax.axis_index("chain"), lax.axis_index("bond"))
    slabs = chains // 2
    slab, core = (chain // 2, chain % 2)
    replica, ring = (bond // RING, order(bond % RING))
    tall = rows * 4
    height = width // CHUNKS
    sibling = {"chain": 2 * slab + 1 - core, "bond": bond}

    def remote(src, dst, send, recv_sem, chain_to, bond_to):
        return pltpu.make_async_remote_copy(
            src_ref=src, dst_ref=dst, send_sem=send, recv_sem=recv_sem,
            device_id={"chain": chain_to, "bond": bond_to},
            device_id_type=pl.DeviceIdType.MESH,
        )

    def landed(ref, sem):
        pltpu.make_async_copy(ref, ref, sem).wait()

    fetch = pltpu.make_async_copy(x_ref, xin, fetch_sem)
    fetch.start()
    gate_here = pltpu.make_async_copy(gates_ref, gates.at[core], gate_recv.at[core])
    gate_here.start()
    barrier = pltpu.get_barrier_semaphore()

    def greet(semaphore, chain_to, bond_to):
        to = {"chain": chain_to, "bond": bond_to}
        pl.semaphore_signal(semaphore, inc=1, device_id=to, device_id_type=pl.DeviceIdType.MESH)

    for db in range(1, bonds):
        greet(barrier, 2 * slab + 1, lax.rem(bond + db, bonds))

    @pl.when(core == 0)
    def _():
        greet(barrier, 2 * slab + 1, bond)

    for dz in range(1, slabs):
        for db in range(RING):
            greet(barrier, 2 * lax.rem(slab + dz, slabs), replica * RING + lax.rem(bond + db, RING))

    @pl.when(core == 1)
    def _():
        pl.semaphore_wait(barrier, 2 * bonds - 1)
        greet(slab_sem, 2 * slab, bond)

    @pl.when(core == 0)
    def _():
        pl.semaphore_wait(slab_sem, 1)

    gate_copy = remote(gates_ref, gates.at[core], gate_send, gate_recv.at[core], sibling["chain"], bond)
    gate_copy.start()
    fetch.wait()

    short = tall // 2
    gathers = []
    for i in (1, 0):
        for h in range(2):
            for j in range(2):
                for r in range(bonds // RING):
                    bond_to = r * RING + order(2 * core + j)
                    src = xin.at[pl.ds((2 * j + i) * tall + h * short, short)]
                    dst = inbuf.at[i, pl.ds(bond * tall + h * short, short)]
                    sem = g_recv.at[i, bond]
                    copy = remote(src, dst, g_send.at[i, h, j, r], sem, 2 * slab + h, bond_to)
                    here = pltpu.make_async_copy(src, dst, sem)
                    mine = jnp.logical_and(core == h, bond_to == bond)
                    gathers.append((copy, mine))
                    pl.when(mine)(here.start)
                    pl.when(jnp.logical_not(mine))(copy.start)

    forwards = []
    part = bonds // 2
    first = bond // part

    def receive(i, origins):
        for origin in origins:
            piece = inbuf.at[i, pl.ds(origin * tall + core * short, short)]
            landed(piece, g_recv.at[i, origin])
            copy = remote(
                piece, piece, f_send.at[i, origin], f_recv.at[i, origin], sibling["chain"], bond
            )
            copy.start()
            forwards.append(copy)
        for origin in origins:
            landed(inbuf.at[i, pl.ds(origin * tall + (1 - core) * short, short)], f_recv.at[i, origin])

    def spin(i, s, row, count):
        return jnp.concatenate(
            [inbuf[i, pl.ds(4 * row + 2 * t + s, count, stride=4), :] for t in range(2)], axis=1
        )

    def meet_ring():
        @pl.when(core == 0)
        def _():
            pl.semaphore_wait(barrier, (slabs - 1) * 2 * RING)
            greet(ring_sem, 2 * slab + 1, bond)

        @pl.when(core == 1)
        def _():
            pl.semaphore_wait(ring_sem, 1)

    passed = []

    def send_left(value):
        for g in range(2):
            for s in range(2):
                here = pl.ds((first + g * (1 - 2 * first)) * half, half)
                xbuf[s, here] = value[(2 * g + s) * half:(2 * g + s + 1) * half]
        before = lax.rem(ring + RING - 1, RING)
        slab_to = lax.rem(slab + slabs - jnp.where(ring == 0, 1, 0), slabs)
        bond_to = replica * RING + order(before)
        for q in range(CHUNKS):
            part = pl.ds(q * height, height)
            copy = remote(
                xbuf.at[core, part], recv.at[core, part], m_send.at[q], m_recv.at[q],
                2 * slab_to + core, bond_to,
            )
            copy.start()
            passed.append(copy)

    block = ring // 2
    half = width // 2

    def left_rows(g):
        which = first + g * (1 - 2 * first)
        receive(0, [which * part + lax.rem(bond + d, part) for d in range(part)])
        return jnp.concatenate([spin(0, s, which * half, half) for s in range(2)], axis=0)

    meet_ring()
    receive(1, [lax.rem(bond + d, bonds) for d in range(bonds)])
    landed(gates.at[0], gate_recv.at[0])
    landed(gates.at[1], gate_recv.at[1])
    right = jnp.concatenate([spin(1, s, 0, width) for s in range(2)], axis=1)
    lefts = [functools.partial(left_rows, g) for g in range(2)]
    new_right, weight_even = update(right, lefts, gates[block, 2 * (ring % 2)], send_left)

    for q in range(CHUNKS):
        part = recv.at[core, pl.ds(q * height, height)]
        landed(part, m_recv.at[q])
        copy = remote(part, part, h_send.at[q], h_recv.at[q], sibling["chain"], bond)
        copy.start()
        forwards.append(copy)
    for q in range(CHUNKS):
        landed(recv.at[1 - core, pl.ds(q * height, height)], h_recv.at[q])

    outs = []

    def put(h, value_of):
        for s in range(2):
            for t in range(2):
                obuf[h, pl.ds(2 * t + s, width, stride=4), :] = value_of(s, t)
        site = lax.rem(slab * 2 * RING + 2 * ring + 1 + h, 4 * chains)
        chain_to, slot = (site // 4, site % 4)
        for j in range(2):
            bond_to = replica * RING + 2 * j + core
            src = obuf.at[h, pl.ds(bond_to * tall, tall)]
            dst = out_ref.at[pl.ds(slot * tall, tall)]
            copy = remote(src, dst, o_send.at[h, j], o_recv.at[slot], chain_to, bond_to)
            here = pltpu.make_async_copy(src, dst, o_recv.at[slot])
            mine = jnp.logical_and(chain_to == chain, bond_to == bond)
            outs.append((copy, mine))
            pl.when(mine)(here.start)
            pl.when(jnp.logical_not(mine))(copy.start)

    def put_left(value):
        put(0, lambda s, t: value[s * width:(s + 1) * width, t * LANES:(t + 1) * LANES])

    left = jnp.concatenate([new_right[:, :width], new_right[:, width:]], axis=0)
    right = jnp.concatenate([recv[0], recv[1]], axis=1)
    new_right, weight_odd = update(right, [lambda: left], gates[block, 2 * (ring % 2) + 1], put_left)

    row = lax.broadcasted_iota(jnp.int32, (8, LANES), 0)
    lane = lax.broadcasted_iota(jnp.int32, (8, LANES), 1)
    own = wall.at[slab * RING + ring]
    own[...] = jnp.where(row == 0, weight_even, weight_odd)
    weights = []
    for dz in range(slabs):
        for dk in range(RING):
            if dz == 0 and dk == 0:
                continue
            chain_to = 2 * lax.rem(slab + dz, slabs) + core
            bond_to = replica * RING + order(lax.rem(ring + dk, RING))
            at = dz * RING + dk
            copy = remote(own, own, w_send.at[at], w_recv.at[at], chain_to, bond_to)
            copy.start()
            weights.append((copy, dz, dk))
    put(1, lambda s, t: new_right[:, s * width + t * LANES:s * width + (t + 1) * LANES])
    for copy, dz, dk in weights:
        source = lax.rem(slab + slabs - dz, slabs) * RING + lax.rem(ring + RING - dk, RING)
        landed(wall.at[source], w_recv.at[dz * RING + dk])
    total = jnp.zeros((8, LANES), jnp.float32)
    for e in range(slabs * RING):
        counted = jnp.logical_and(row < 2, 2 * e + row <= 4 * chain + lane)
        total = total + jnp.where(counted, wall[e], 0.0)
    running = jnp.sum(total, axis=0, keepdims=True) * (1.0 / (4 * chains))
    profile_ref[...] = jnp.broadcast_to(running, (8, LANES))

    for slot in range(4):
        landed(out_ref.at[pl.ds(slot * tall, tall)], o_recv.at[slot])
    for copy, mine in gathers:
        pl.when(jnp.logical_not(mine))(copy.wait_send)
    gate_copy.wait_send()
    for copy in forwards + passed + [c for c, dz, dk in weights]:
        copy.wait_send()
    for copy, mine in outs:
        pl.when(jnp.logical_not(mine))(copy.wait_send)


def per_device(chains, bonds, site_tensors, bond_gates):
    sites, rows, spins, width = site_tensors.shape
    assert sites == 4 and spins == 2 and width == 2 * LANES and bonds % RING == 0 and chains % 2 == 0
    cut = (sites, rows, spins, width // LANES, LANES)
    flat = site_tensors.reshape(cut).transpose(0, 1, 3, 2, 4).reshape(sites * rows * 4, LANES)
    slabs = chains // 2
    dma = pltpu.SemaphoreType.DMA
    out, profile = pl.pallas_call(
        functools.partial(kernel, chains, bonds, rows, width),
        out_shape=(
            jax.ShapeDtypeStruct(flat.shape, jnp.float32),
            jax.ShapeDtypeStruct((8, LANES), jnp.float32),
        ),
        in_specs=[pl.BlockSpec(memory_space=pltpu.HBM)] * 2,
        out_specs=(pl.BlockSpec(memory_space=pl.ANY), pl.BlockSpec(memory_space=pltpu.VMEM)),
        scratch_shapes=[
            pltpu.SemaphoreType.REGULAR,
            pltpu.SemaphoreType.REGULAR,
            dma,
            pltpu.VMEM(flat.shape, jnp.float32),
            pltpu.VMEM((2, 4 * width, LANES), jnp.float32),
            pltpu.VMEM((2,) + bond_gates.shape, jnp.float32),
            pltpu.VMEM((2, width, width), jnp.float32),
            pltpu.VMEM((2, width, width), jnp.float32),
            pltpu.VMEM((2, 4 * width, LANES), jnp.float32),
            pltpu.VMEM((slabs * RING, 8, LANES), jnp.float32),
            dma((2, 2, 2, bonds // RING)), dma((2, bonds)),
            dma((2, bonds)), dma((2, bonds)),
            dma, dma((2,)),
            dma((CHUNKS,)), dma((CHUNKS,)),
            dma((CHUNKS,)), dma((CHUNKS,)),
            dma((2, 2)), dma((4,)),
            dma((slabs * RING,)), dma((slabs * RING,)),
        ],
        compiler_params=pltpu.CompilerParams(
            has_side_effects=True, collective_id=0, vmem_limit_bytes=56_000_000
        ),
    )(flat, bond_gates)
    cut = (sites, rows, width // LANES, spins, LANES)
    state = out.reshape(cut).transpose(0, 1, 3, 2, 4).reshape(site_tensors.shape)
    return (state, profile[0, :sites])


def solution(mesh):
    chains, bonds = (mesh.shape["chain"], mesh.shape["bond"])
    return jax.shard_map(
        functools.partial(per_device, chains, bonds),
        mesh=mesh,
        in_specs=(P("chain", "bond", None, None), P("chain", None, None)),
        out_specs=(P("chain", "bond", None, None), P("chain")),
        check_vma=False,
    )
```
